256 devices in a mesh: node: 32 (over x, z_hi, core), local: 8 (over z_lo, y).
Axes of the slice: x: 4, y: 4, z: 8 (z_hi: 4, z_lo: 2; z = z_hi * 2 + z_lo), core: 2. Of those that a mesh axis runs over, the one named last changes fastest.
Arguments:
- hidden: bfloat16 [8, 8192, 4096], P('local', 'node'), may hold values from -6 to 6
- queries: bfloat16 [8, 8192, 2048], P('local', 'node'), may hold values from -30 to 30
- saved_keys: bfloat16 [8, 8192, 512], P('local', 'node'), may hold values from -30 to 30
- grad_out: bfloat16 [8, 8192, 2048], P('local', 'node'), may hold values from -6 to 6
- value_weight: bfloat16 [4096, 512], P('local'), may hold values from -0.09375 to 0.09375
- doc_lengths: int32 [8, 32], P('local'), may hold values from 0 to 1024, as said below
- doc_order: int32 [8, 32], P('local'), may hold values from 0 to 31, each once within a row
Outputs:
- query_grad: bfloat16 [8, 8192, 2048], P('local', 'node')
- key_grad: bfloat16 [8, 8192, 512], P('local', 'node')
- input_grad: bfloat16 [8, 8192, 4096], P('local', 'node')
- weight_grad: float32 [4096, 512], P(('node', 'local'))
The draws below stay inside these ranges and needn't reach their ends.
Inputs may be any that keep to these rules, and one draw needn't show every extreme that they name: `doc_lengths`: a document occupies ceil(length / 256) whole blocks, at most 4; the documents of a sequence fill its 32 blocks exactly; in every sequence some document takes 4 blocks.
All inputs are finite; a program needn't handle non-finite values.
Results may differ from the reference program's by a relative error of at most 0.0085.
Values may be sent and summed in bfloat16 or wider, within the bound.
No kernel may reach another device: no remote copies, remote signals or barrier semaphores. Data moves between devices by JAX's collectives and lax.ppermute only.
A program may use at most 128 MiB of HBM per device.

```python
import jax
import jax.numpy as jnp
from jax import lax

D = 4096
HD = 128
KVH = 4
GROUP = 4
BLOCK = 256
DOCB = 4
QW = 2048
KVW = 512
NBLK = 32
SEQLEN = 8192
SEQS = 8


def paired_rows(key):
    base = jax.random.fold_in(key, 17)
    key_query, key_keys = jax.random.split(base)
    query_draw = jnp.clip(jax.random.normal(key_query, (SEQS, SEQLEN, QW), jnp.float32), -6.0, 6.0)
    key_draw = jnp.clip(jax.random.normal(key_keys, (SEQS, SEQLEN, KVW), jnp.float32), -6.0, 6.0)
    return (query_draw, key_draw)


def draw_queries(key, part):
    return paired_rows(key)[0].astype(jnp.bfloat16)


def draw_saved_keys(key, part):
    return paired_rows(key)[1].astype(jnp.bfloat16)


def draw_doc_lengths(key, part):
    key_count, key_len = jax.random.split(jax.random.fold_in(key, 3))
    counts = jax.random.randint(key_count, (SEQS, NBLK), 1, DOCB + 1)
    counts = counts.at[:, 1].set(DOCB)
    ends = jnp.cumsum(counts, axis=1)
    starts = ends - counts
    living = starts < NBLK
    counts = jnp.where(living, jnp.minimum(counts, NBLK - starts), 0)
    extra = jax.random.randint(key_len, (SEQS, NBLK), 1, BLOCK + 1)
    return jnp.where(living, (counts - 1) * BLOCK + extra, 0).astype(jnp.int32)


def strengthened(values, key, source, target, parts, factor):
    def block_of(position):
        return (jnp.arange(values.shape[position]) // (values.shape[position] // parts)).reshape((-1,) + (1,) * (values.ndim - 1 - position))

    near = jax.random.permutation(key, parts)[block_of(target)]
    second = (block_of(target) + parts // 2) % parts
    return jnp.where((block_of(source) == near) | (block_of(source) == second), factor * values, values)


def block_scale(rng, dims, cuts, smallest, largest):
    loudness, own = 1.0, jax.random.fold_in(rng, 6)
    for dim, parts in cuts:
        draws = jnp.exp(jax.random.uniform(jax.random.fold_in(own, dim), (parts,), jnp.float32, smallest / len(cuts), largest / len(cuts)))
        loudness = loudness * jnp.repeat(draws, dims[dim] // parts).reshape([-1 if axis == dim else 1 for axis in range(len(dims))])
    return loudness


def normal_values(stream_key, extent, spread, limit, shards=(), held_as=jnp.bfloat16):
    gain = block_scale(stream_key, extent, shards, -0.22, 0.18) if shards else 1.0
    entries = jax.random.normal(stream_key, extent, jnp.float32) * spread * gain
    return jnp.minimum(jnp.maximum(entries, -limit), limit).astype(held_as)


def gaussian_with(key, shape, deviation, most, cuts, heavy, kind=jnp.bfloat16):
    result = deviation * jax.random.normal(key, shape, jnp.float32)
    if cuts:
        result = result * block_scale(key, shape, cuts, -0.22, 0.18)
    return jnp.clip(strengthened(result, jax.random.fold_in(key, 3), *heavy), -most, most).astype(kind)


def setup_inputs(seed: int = 0) -> dict:
    arg_keys = jax.random.split(jax.random.key(seed), 8)
    hidden = gaussian_with(arg_keys[0], (SEQS, SEQLEN, D), 1.0, 6.0, ((0, 8), (1, 32)), (1, 2, 32, 2.75))
    queries = draw_queries(jax.random.fold_in(arg_keys[7], 71), 0)
    saved_keys = draw_saved_keys(jax.random.fold_in(arg_keys[7], 71), 0)
    grad_out = normal_values(arg_keys[3], (SEQS, SEQLEN, QW), 1.0, 6.0, ((0, 8), (1, 32)))
    value_weight = normal_values(arg_keys[4], (D, KVW), D ** -0.5, 0.09375, ((0, 8),))
    doc_lengths = draw_doc_lengths(jax.random.fold_in(arg_keys[7], 71), 0)
    doc_order = jax.vmap(lambda own: jax.random.permutation(own, NBLK))(jax.random.split(arg_keys[6], SEQS)).reshape((SEQS, NBLK)).astype(jnp.int32)
    return {"hidden": hidden, "queries": queries, "saved_keys": saved_keys, "grad_out": grad_out, "value_weight": value_weight, "doc_lengths": doc_lengths, "doc_order": doc_order}


masked_score = -1e30


def doc_layout(lengths_row, order_row):
    slot_ids = jnp.arange(NBLK, dtype=jnp.int32)
    picked = order_row[:, None] == slot_ids[None, :]
    lens_ord = jnp.sum(jnp.where(picked, lengths_row[None, :], 0), axis=1).astype(jnp.int32)
    block_count = ((lens_ord + BLOCK - 1) // BLOCK).astype(jnp.int32)
    first_block = (jnp.cumsum(block_count) - block_count).astype(jnp.int32)
    return lens_ord, block_count, first_block


def block_info(block_index, lens_ord, block_count, first_block):
    member = (first_block <= block_index) & (block_index < first_block + block_count)
    has_doc = jnp.any(member)
    doc_start = jnp.sum(jnp.where(member, first_block, 0)).astype(jnp.int32)
    length = jnp.sum(jnp.where(member, lens_ord, 0)).astype(jnp.int32)
    return jnp.where(has_doc, doc_start, -1).astype(jnp.int32), length


def window_mask(block_index, layout):
    doc_start, length = block_info(block_index, *layout)
    inside = jnp.arange(BLOCK, dtype=jnp.int32)
    query_ok = (block_index - doc_start) * BLOCK + inside < length
    mask_parts = []
    for offset in range(DOCB - 1, -1, -1):
        other_block = block_index - offset
        other_start, other_len = block_info(other_block, *layout)
        key_ok = (other_start == doc_start) & ((other_block - doc_start) * BLOCK + inside < length)
        allowed = jnp.broadcast_to(key_ok[None, :], (BLOCK, BLOCK))
        if offset == 0:
            allowed = allowed & (inside[None, :] <= inside[:, None])
        mask_parts.append(allowed)
    return query_ok, jnp.concatenate(mask_parts, axis=1)


def tile_grads(query_rows, grad_rows, key_window, value_window, allowed):
    width = key_window.shape[0]
    score_scale = HD ** -0.5
    q_heads = query_rows.reshape(BLOCK, KVH, GROUP, HD).astype(jnp.float32)
    g_heads = grad_rows.reshape(BLOCK, KVH, GROUP, HD).astype(jnp.float32)
    k_heads = key_window.reshape(width, KVH, HD).astype(jnp.float32)
    v_heads = value_window.reshape(width, KVH, HD).astype(jnp.float32)
    scores = jnp.einsum("tgjd,wgd->gjtw", q_heads, k_heads) * score_scale
    scores = jnp.where(allowed[None, None], scores, masked_score)
    peak = jnp.max(scores, axis=3, keepdims=True)
    expd = jnp.exp(scores - peak)
    attn_probs = expd / jnp.sum(expd, axis=3, keepdims=True)
    attn_low = attn_probs.astype(jnp.bfloat16).astype(jnp.float32)
    attn_out = jnp.einsum("gjtw,wgd->tgjd", attn_low, v_heads)
    prob_grad = jnp.einsum("tgjd,wgd->gjtw", g_heads, v_heads)
    row_delta = jnp.einsum("tgjd,tgjd->gjt", g_heads, attn_out)
    score_grad = (attn_probs * (prob_grad - row_delta[..., None]) * score_scale).astype(jnp.bfloat16).astype(jnp.float32)
    query_grad = jnp.einsum("gjtw,wgd->tgjd", score_grad, k_heads).reshape(BLOCK, QW).astype(jnp.bfloat16)
    key_grad = jnp.einsum("gjtw,tgjd->wgd", score_grad, q_heads).reshape(width, KVW)
    value_grad = jnp.einsum("gjtw,tgjd->wgd", attn_low, g_heads).reshape(width, KVW)
    return query_grad, key_grad, value_grad


def gather_window(windows):
    pieces = windows.reshape(NBLK, DOCB, BLOCK, KVW)
    summed = jnp.zeros((NBLK + DOCB - 1, BLOCK, KVW), jnp.float32)
    for offset in range(DOCB):
        summed = summed.at[offset:offset + NBLK].add(pieces[:, offset])
    return summed[DOCB - 1:].reshape(SEQLEN, KVW)


def reference(hidden, queries, saved_keys, grad_out, value_weight, doc_lengths, doc_order):
    flat_hidden = hidden.reshape(SEQS * SEQLEN, D)
    values = jnp.dot(flat_hidden, value_weight, preferred_element_type=jnp.float32).astype(jnp.bfloat16)
    values = values.reshape(SEQS, SEQLEN, KVW)
    query_list, key_list, value_list = [], [], []
    for sequence in range(SEQS):
        layout = doc_layout(doc_lengths[sequence], doc_order[sequence])
        padding = jnp.zeros(((DOCB - 1) * BLOCK, KVW), jnp.bfloat16)
        key_padded = jnp.concatenate([padding, saved_keys[sequence]], axis=0)
        value_padded = jnp.concatenate([padding, values[sequence]], axis=0)
        seq_queries = queries[sequence]
        seq_grads = grad_out[sequence]

        def one_block(block_index):
            query_ok, allowed = window_mask(block_index, layout)
            first_row = (block_index * BLOCK).astype(jnp.int32)
            query_rows = lax.dynamic_slice_in_dim(seq_queries, first_row, BLOCK, 0)
            grad_rows = lax.dynamic_slice_in_dim(seq_grads, first_row, BLOCK, 0)
            grad_rows = grad_rows * query_ok[:, None].astype(grad_rows.dtype)
            key_window = lax.dynamic_slice_in_dim(key_padded, first_row, DOCB * BLOCK, 0)
            value_window = lax.dynamic_slice_in_dim(value_padded, first_row, DOCB * BLOCK, 0)
            return tile_grads(query_rows, grad_rows, key_window, value_window, allowed)

        block_query, block_key, block_value = lax.map(one_block, jnp.arange(NBLK, dtype=jnp.int32))
        query_list.append(block_query.reshape(SEQLEN, QW))
        key_list.append(gather_window(block_key))
        value_list.append(gather_window(block_value))
    query_grad = jnp.stack(query_list)
    key_grad = jnp.stack(key_list).astype(jnp.bfloat16)
    value_low = jnp.stack(value_list).astype(jnp.bfloat16).reshape(SEQS * SEQLEN, KVW)
    input_grad = jnp.dot(value_low, value_weight.T, preferred_element_type=jnp.float32).astype(jnp.bfloat16)
    weight_grad = jnp.dot(flat_hidden.T, value_low, preferred_element_type=jnp.float32)
    return query_grad, key_grad, input_grad.reshape(SEQS, SEQLEN, D), weight_grad
```

```python
import functools

import jax
import jax.numpy as jnp
from jax import lax
from jax.experimental import pallas as pl
from jax.experimental.pallas import tpu as pltpu
from jax.sharding import Mesh, PartitionSpec as P

HD = 128
GROUP = 4
KVH = 4
BLK = 256
DOCB = 4
SCALE = HD**-0.5
EXP2_SCALE = SCALE * 1.4426950408889634
BF = jnp.bfloat16
F32 = jnp.float32

NODE = ("x", "h", "c")
LOCAL = ("l", "y")


def dot(a, b, ca, cb):
    return lax.dot_general(a, b, (((ca,), (cb,)), ((), ())), preferred_element_type=F32)


def node_shift(block, pairs):
    return lax.ppermute(block, NODE, pairs)


def core_swap(block):
    return lax.ppermute(block, "c", [(0, 1), (1, 0)])


def window_in(block, nodes):
    behind2 = node_shift(block, [(i, i + 2) for i in range(nodes - 2)])
    behind3 = node_shift(behind2, [(i, i + 1) for i in range(1, nodes - 1, 2)])
    swapped = core_swap(jnp.stack([block, behind2]))
    return behind2, behind3, swapped


def window_out(own, two, sent, core, nodes):
    swapped = core_swap(sent)
    first = core == 0
    own = own + jnp.where(first, swapped[0], jnp.zeros_like(swapped[0])).astype(F32)
    two = two + jnp.where(first, swapped[1], swapped[0]).astype(F32)
    passed = node_shift(swapped[1], [(i, i - 2) for i in range(3, nodes, 2)])
    two = (two + passed.astype(F32)).astype(BF)
    got = node_shift(two, [(i, i - 2) for i in range(2, nodes)])
    return (own + got.astype(F32)).astype(BF)


def find_doc(node, lens_ref, order_ref):
    slots = lens_ref.shape[1]

    def step(j, carry):
        start, doc_start, length = carry
        own = lens_ref[0, order_ref[0, j]]
        count = (own + (BLK - 1)) >> 8
        inside = (start <= node) & (node < start + count)
        doc_start = jnp.where(inside, start, doc_start)
        length = jnp.where(inside, own, length)
        return start + count, doc_start, length

    zero = jnp.int32(0)
    _, doc_start, length = lax.fori_loop(0, slots, step, (zero, zero, zero))
    before = node - doc_start
    return before, length - before * BLK


def fill_window(core, own, two, three, swapped, win):
    win[0:BLK] = own[...]
    win[2 * BLK : 3 * BLK] = two[...]

    @pl.when(core == 0)
    def _():
        win[BLK : 2 * BLK] = swapped[1]
        win[3 * BLK : 4 * BLK] = three[...]

    @pl.when(core != 0)
    def _():
        win[BLK : 2 * BLK] = swapped[0]
        win[3 * BLK : 4 * BLK] = swapped[1]


def stack_heads(src, dst, mask=None):
    for j in range(GROUP):
        cols = src[:, j * HD : (j + 1) * HD]
        dst[j * BLK : (j + 1) * BLK] = cols if mask is None else cols * mask


def row_mask(real):
    rows = lax.broadcasted_iota(jnp.int32, (BLK, HD), 0)
    return jnp.where(rows < real, 1.0, 0.0).astype(BF)


def probs_kernel(
    where_ref, lens_ref, order_ref, q_ref, g_ref, k0, k2, k3, ks,
    p_ref, dv0_ref, dv2_ref, dvs_ref, kwin, qst, gst, info,
):
    core = where_ref[1]

    @pl.when(pl.program_id(0) == 0)
    def _():
        before, real = find_doc(where_ref[0], lens_ref, order_ref)
        info[0] = before
        info[1] = real

    before = info[0]
    fill_window(core, k0, k2, k3, ks, kwin)
    stack_heads(q_ref, qst)
    stack_heads(g_ref, gst, row_mask(info[1]))
    key_id = lax.broadcasted_iota(jnp.int32, (BLK, BLK), 0)
    query_id = lax.broadcasted_iota(jnp.int32, (BLK, BLK), 1)
    causal = key_id <= query_id
    for j in range(GROUP):
        qj = qst[j * BLK : (j + 1) * BLK]
        scores = [dot(kwin[w * BLK : (w + 1) * BLK], qj, 1, 1) for w in range(DOCB)]
        scores[0] = jnp.where(causal, scores[0], -1e30)
        peaks = [jnp.max(s, axis=0, keepdims=True) for s in scores]
        peak = peaks[0]
        for w in range(1, DOCB):
            peak = jnp.maximum(peak, jnp.where(before >= w, peaks[w], -1e30))
        total = jnp.zeros((1, BLK), F32)
        expd = []
        for w in range(DOCB):
            base = peak if w == 0 else jnp.where(before >= w, peak, 1e30)
            e = jnp.exp2((scores[w] - base) * EXP2_SCALE)
            total = total + jnp.sum(e, axis=0, keepdims=True)
            expd.append(e)
        inv = 1.0 / total
        for w in range(DOCB):
            p_ref[0, w * BLK : (w + 1) * BLK, j * BLK : (j + 1) * BLK] = (expd[w] * inv).astype(BF)
    terms = [dot(p_ref[0, w * BLK : (w + 1) * BLK, :], gst[...], 1, 0) for w in range(DOCB)]
    dv0_ref[...] = terms[0]
    dv2_ref[...] = terms[2]
    dvs_ref[0] = terms[1].astype(BF)
    dvs_ref[1] = terms[3].astype(BF)


def grads_kernel(
    where_ref, lens_ref, order_ref, q_ref, g_ref, k0, k2, k3, ks, v0, v2, v3, vs, p_ref,
    dq_ref, dk0_ref, dk2_ref, dks_ref, kwin, vwin, qst, gst, dst, info,
):
    core = where_ref[1]

    @pl.when(pl.program_id(0) == 0)
    def _():
        _, real = find_doc(where_ref[0], lens_ref, order_ref)
        info[0] = real

    fill_window(core, k0, k2, k3, ks, kwin)
    fill_window(core, v0, v2, v3, vs, vwin)
    stack_heads(q_ref, qst)
    stack_heads(g_ref, gst, row_mask(info[0]))
    key_t = jnp.transpose(kwin[...])
    for j in range(GROUP):
        gj = gst[j * BLK : (j + 1) * BLK]
        delta = jnp.zeros((1, BLK), F32)
        grads = []
        for w in range(DOCB):
            pg = dot(vwin[w * BLK : (w + 1) * BLK], gj, 1, 1)
            p = p_ref[0, w * BLK : (w + 1) * BLK, j * BLK : (j + 1) * BLK].astype(F32)
            delta = delta + jnp.sum(p * pg, axis=0, keepdims=True)
            grads.append(pg)
        for w in range(DOCB):
            p = p_ref[0, w * BLK : (w + 1) * BLK, j * BLK : (j + 1) * BLK].astype(F32)
            dst[w * BLK : (w + 1) * BLK, j * BLK : (j + 1) * BLK] = (p * (grads[w] - delta)).astype(BF)
        dq_t = dot(key_t, dst[:, j * BLK : (j + 1) * BLK], 1, 0) * SCALE
        dq_ref[:, j * HD : (j + 1) * HD] = jnp.transpose(dq_t).astype(BF)
    terms = [dot(dst[w * BLK : (w + 1) * BLK, :], qst[...], 1, 0) * SCALE for w in range(DOCB)]
    dk0_ref[...] = terms[0]
    dk2_ref[...] = terms[2]
    dks_ref[0] = terms[1].astype(BF)
    dks_ref[1] = terms[3].astype(BF)


SMEM = pl.BlockSpec(memory_space=pltpu.SMEM)
HEADS = pl.BlockSpec((BLK, GROUP * HD), lambda g: (0, g))
ONE = pl.BlockSpec((BLK, HD), lambda g: (0, g))
PAIR = pl.BlockSpec((2, BLK, HD), lambda g: (0, 0, g))
PROBS = pl.BlockSpec((1, DOCB * BLK, GROUP * BLK), lambda g: (g, 0, 0))
KVW = KVH * HD
TERMS = (
    jax.ShapeDtypeStruct((BLK, KVW), F32),
    jax.ShapeDtypeStruct((BLK, KVW), F32),
    jax.ShapeDtypeStruct((2, BLK, KVW), BF),
)


def run_probs(where, lens, order, q, g, k0, k2, k3, ks):
    return pl.pallas_call(
        probs_kernel,
        grid=(KVH,),
        in_specs=[SMEM, SMEM, SMEM, HEADS, HEADS, ONE, ONE, ONE, PAIR],
        out_specs=(PROBS, ONE, ONE, PAIR),
        out_shape=(jax.ShapeDtypeStruct((KVH, DOCB * BLK, GROUP * BLK), BF),) + TERMS,
        scratch_shapes=[
            pltpu.VMEM((DOCB * BLK, HD), BF),
            pltpu.VMEM((GROUP * BLK, HD), BF),
            pltpu.VMEM((GROUP * BLK, HD), BF),
            pltpu.SMEM((2,), jnp.int32),
        ],
        name="probs",
    )(where, lens, order, q, g, k0, k2, k3, ks)


def run_grads(where, lens, order, q, g, k0, k2, k3, ks, v0, v2, v3, vs, probs):
    return pl.pallas_call(
        grads_kernel,
        grid=(KVH,),
        in_specs=[SMEM, SMEM, SMEM, HEADS, HEADS] + [ONE, ONE, ONE, PAIR] * 2 + [PROBS],
        out_specs=(HEADS, ONE, ONE, PAIR),
        out_shape=(jax.ShapeDtypeStruct(q.shape, BF),) + TERMS,
        scratch_shapes=[
            pltpu.VMEM((DOCB * BLK, HD), BF),
            pltpu.VMEM((DOCB * BLK, HD), BF),
            pltpu.VMEM((GROUP * BLK, HD), BF),
            pltpu.VMEM((GROUP * BLK, HD), BF),
            pltpu.VMEM((DOCB * BLK, GROUP * BLK), BF),
            pltpu.SMEM((1,), jnp.int32),
        ],
        name="grads",
    )(where, lens, order, q, g, k0, k2, k3, ks, v0, v2, v3, vs, probs)


def split_kernel(where_ref, x_ref, keep_ref, send_ref):
    even = jnp.transpose(x_ref[:, :HD])
    odd = jnp.transpose(x_ref[:, HD:])

    @pl.when(where_ref[1] == 0)
    def _():
        keep_ref[...] = even
        send_ref[...] = odd

    @pl.when(where_ref[1] != 0)
    def _():
        keep_ref[...] = odd
        send_ref[...] = even


def split_columns(where, x):
    rows, width = x.shape
    half = jax.ShapeDtypeStruct((width // 2, rows), BF)
    out = pl.BlockSpec((HD, rows), lambda i: (i, 0))
    return pl.pallas_call(
        split_kernel,
        grid=(width // (2 * HD),),
        in_specs=[SMEM, pl.BlockSpec((rows, 2 * HD), lambda i: (0, i))],
        out_specs=(out, out),
        out_shape=(half, half),
        name="split",
    )(where, x)


def values_kernel(where_ref, x_ref, wa_ref, wb_ref, out_ref, acc_a, acc_b):
    step = pl.program_id(0)

    @pl.when(step == 0)
    def _():
        acc_a[...] = jnp.zeros_like(acc_a)
        acc_b[...] = jnp.zeros_like(acc_b)

    acc_a[...] += dot(x_ref[...], wa_ref[...], 1, 0)
    acc_b[...] += dot(x_ref[...], wb_ref[...], 1, 0)
    half = acc_a.shape[1]

    @pl.when(step == pl.num_programs(0) - 1)
    def _():
        a, b = acc_a[...].astype(BF), acc_b[...].astype(BF)

        @pl.when(where_ref[1] == 0)
        def _():
            out_ref[:, :half] = a
            out_ref[:, half:] = b

        @pl.when(where_ref[1] != 0)
        def _():
            out_ref[:, :half] = b
            out_ref[:, half:] = a


def run_values(where, x, wa, wb):
    rows, width = x.shape
    half = wa.shape[1]
    piece = 1024
    weight = pl.BlockSpec((piece, half), lambda i: (i, 0))
    return pl.pallas_call(
        values_kernel,
        grid=(width // piece,),
        in_specs=[SMEM, pl.BlockSpec((rows, piece), lambda i: (0, i)), weight, weight],
        out_specs=pl.BlockSpec((rows, 2 * half), lambda i: (0, 0)),
        out_shape=jax.ShapeDtypeStruct((rows, 2 * half), BF),
        scratch_shapes=[pltpu.VMEM((rows, half), F32), pltpu.VMEM((rows, half), F32)],
        name="values",
    )(where, x, wa, wb)


def input_grad_kernel(where_ref, v_ref, wa_ref, wb_ref, out_ref, va, vb):
    half = va.shape[1]

    @pl.when(pl.program_id(0) == 0)
    def _():
        @pl.when(where_ref[1] == 0)
        def _():
            va[...] = v_ref[:, :half]
            vb[...] = v_ref[:, half:]

        @pl.when(where_ref[1] != 0)
        def _():
            va[...] = v_ref[:, half:]
            vb[...] = v_ref[:, :half]

    out = dot(va[...], wa_ref[...], 1, 1) + dot(vb[...], wb_ref[...], 1, 1)
    out_ref[...] = out.astype(BF)


def run_input_grad(where, v, wa, wb):
    rows = v.shape[0]
    width, half = wa.shape
    piece = 1024
    weight = pl.BlockSpec((piece, half), lambda i: (i, 0))
    return pl.pallas_call(
        input_grad_kernel,
        grid=(width // piece,),
        in_specs=[SMEM, pl.BlockSpec(v.shape, lambda i: (0, 0)), weight, weight],
        out_specs=pl.BlockSpec((rows, piece), lambda i: (0, i)),
        out_shape=jax.ShapeDtypeStruct((rows, width), BF),
        scratch_shapes=[pltpu.VMEM((rows, half), BF), pltpu.VMEM((rows, half), BF)],
        name="input_grad",
    )(where, v, wa, wb)


def weight_grad_kernel(xa_ref, xb_ref, va_ref, vb_ref, out_ref):
    part = dot(xa_ref[...], va_ref[...], 1, 0) + dot(xb_ref[...], vb_ref[...], 1, 0)
    part = part.astype(BF)
    for h in range(4):
        for l in range(2):
            for y in range(4):
                row = ((h * 2 + l) * 4 + y) * 16
                out_ref[0, y, h * 2 + l] = part[row : row + 16]


def run_weight_grad(xa, xb, va, vb):
    rows, tokens = xa.shape
    width = va.shape[1]
    piece = rows // 4
    x_spec = pl.BlockSpec((piece, tokens), lambda i: (i, 0))
    v_spec = pl.BlockSpec(va.shape, lambda i: (0, 0))
    return pl.pallas_call(
        weight_grad_kernel,
        grid=(4,),
        in_specs=[x_spec, x_spec, v_spec, v_spec],
        out_specs=pl.BlockSpec((1, 4, 8, 16, width), lambda i: (i, 0, 0, 0, 0)),
        out_shape=jax.ShapeDtypeStruct((4, 4, 8, 16, width), BF),
        name="weight_grad",
    )(xa, xb, va, vb)


def exchanged(pieces, axes):
    return lax.all_to_all(pieces, axes, split_axis=0, concat_axis=0, tiled=True)


def local(hidden, queries, saved_keys, grad_out, value_weight, lens, order):
    node = lax.axis_index(NODE).astype(jnp.int32)
    core = lax.axis_index("c").astype(jnp.int32)
    nodes = lax.axis_size(NODE)
    where = jnp.stack([node, core])
    x, q, k, g = hidden[0], queries[0], saved_keys[0], grad_out[0]

    k2, k3, ks = window_in(k, nodes)

    half = value_weight.shape[1] // 2
    mine = lax.dynamic_slice_in_dim(value_weight, core * half, half, 1)
    group = lax.axis_size(LOCAL)
    weight_a = exchanged(jnp.broadcast_to(mine[None], (group,) + mine.shape), LOCAL)
    weight_a = weight_a.reshape(-1, half)
    weight_b = core_swap(weight_a)

    kept, sent = split_columns(where, x)
    brought = core_swap(sent)

    probs, dv0, dv2, dvs = run_probs(where, lens, order, q, g, k, k2, k3, ks)
    values = run_values(where, x, weight_a, weight_b)
    v2, v3, vs = window_in(values, nodes)
    value_low = window_out(dv0, dv2, dvs, core, nodes)

    part = run_weight_grad(kept, brought, value_low, core_swap(value_low))
    part = exchanged(part.reshape(16, 128, -1), ("x", "y"))
    part = part.astype(F32).sum(axis=0).astype(BF)
    part = exchanged(part.reshape(8, 16, -1), ("h", "l"))
    weight_grad = part.astype(F32).sum(axis=0)

    query_grad, dk0, dk2, dks = run_grads(
        where, lens, order, q, g, k, k2, k3, ks, values, v2, v3, vs, probs
    )
    key_grad = window_out(dk0, dk2, dks, core, nodes)
    input_grad = run_input_grad(where, value_low, weight_a, weight_b)
    return query_grad[None], key_grad[None], input_grad[None], weight_grad


def solution(mesh):
    parts = Mesh(mesh.devices.reshape(4, 4, 2, 2, 4), ("x", "h", "c", "l", "y"))
    rows = P(LOCAL, NODE, None)
    return jax.shard_map(
        local,
        mesh=parts,
        in_specs=(rows, rows, rows, rows, P(LOCAL, None), P(LOCAL, None), P(LOCAL, None)),
        out_specs=(rows, rows, rows, P(NODE + LOCAL, None)),
        check_vma=False,
    )
```
